128 devices in a mesh: row: 8 (over x, core), col: 16 (over y, z).
Axes of the slice: x: 4, y: 4, z: 4, core: 2. Of those that a mesh axis runs over, the one named last changes fastest.
Arguments:
- tokens: bfloat16 [65536, 1024], P(('row', 'col')), may hold values from -6 to 6
- expert_ids: int32 [65536, 1], P(('row', 'col')), may hold values from 0 to 127; in each aligned block of 512 rows (0 to 511, 512 to 1023, ...) at most 8 rows name the same one
- gate_prob: float32 [65536], P(('row', 'col')), may hold values from 0.25 to 1
- norm_gain: float32 [1024], replicated, may hold values from 0.1 to 1.9
- weight_in: bfloat16 [128, 1024, 4096], P(('row', 'col')), may hold values from -0.1875 to 0.1875
- weight_out: bfloat16 [128, 4096, 1024], P(('row', 'col')), may hold values from -0.09375 to 0.09375
Outputs:
- mixed: bfloat16 [65536, 1024], P(('row', 'col'))
- routed: int32 [128], P(('row', 'col'))
The draws below stay inside these ranges and needn't reach their ends.
Inputs may be any that keep to these rules, and one draw needn't show every extreme that they name: `expert_ids`: among the 512 tokens of one device no expert is chosen more than 8 times; some expert is chosen exactly 8 times by some device's tokens.
All inputs are finite; a program needn't handle non-finite values.
Results may differ from the reference program's by a relative error of at most 0.001.
The reference program's roundings to bfloat16 on the way (of `normed`, `slots`, `hidden` and `answers`) count: a program that leaves them out, or rounds other values in their place, can miss the bound.
Values may be sent and summed in bfloat16 or wider, within the bound.
A program may use at most 64 MiB of HBM per device.

```python
import math
import jax
import jax.numpy as jnp
import numpy as np
from jax import lax

D = 1024
FF = 4096
TOK_DEV = 512
EXPERTS = 128
CAP = 8
TOKENS = 65536
DEVICES = 128


def draw_tokens(key, part):
    base_key = jax.random.fold_in(key, 11)
    value_key, sparse_key, choose_key = jax.random.split(base_key, 3)
    values = jnp.clip(jax.random.normal(value_key, (TOKENS, D), jnp.float32), -6.0, 6.0)
    sparse_rows = jax.random.randint(sparse_key, (TOKENS,), 0, 64) == 0
    chosen = jax.random.randint(choose_key, (TOKENS // TOK_DEV,), 0, TOK_DEV)
    position = jnp.arange(TOKENS, dtype=jnp.int32)
    block_index = position // TOK_DEV
    forced_rows = position % TOK_DEV == chosen[block_index]
    kept_rows = jnp.logical_not(jnp.logical_or(sparse_rows, forced_rows)).astype(jnp.float32)
    return (values * kept_rows[:, None]).astype(jnp.bfloat16)


def levels(key, dims, cuts, low, high):
    level, own = 1.0, jax.random.fold_in(key, 6)
    for dim, parts in cuts:
        steps = jnp.exp(jax.random.uniform(jax.random.fold_in(own, dim), (parts,), jnp.float32, low / len(cuts), high / len(cuts)))
        level = level * jnp.repeat(steps, dims[dim] // parts).reshape([-1 if axis == dim else 1 for axis in range(len(dims))])
    return level


def routed_block(own_key, own, number, rows, number_of, top, reach, lean):
    order = jax.random.permutation(own_key, number_of)
    heavy_load, usual = portions_of(number_of, rows * top, reach, lean, True), portions_of(number_of, rows * top, reach, lean, False)
    places = jnp.arange(number_of)

    def named(tallies, offset_by):
        used = int((tallies > 0).sum())
        fixed = max(1, used // 4)
        moved = fixed + (places - fixed + offset_by * (used - fixed)) % max(1, number_of - fixed)
        return jnp.zeros((number_of,), jnp.int32).at[order[jnp.where(places < fixed, places, moved)]].set(jnp.asarray(tallies, jnp.int32))

    tallies = jnp.where(number % 4 == 0, named(heavy_load, number // 4), named(usual, number - number // 4 - 1))
    mixed = jax.random.permutation(jax.random.fold_in(own, 3), number_of)
    donor, sink = mixed[0:number_of // 2 * 2:2], mixed[1:number_of // 2 * 2:2]
    room = jnp.minimum(tallies[donor] - 1, reach - tallies[sink]) // 2
    room = jnp.where((donor == order[0]) | (sink == order[0]) | (tallies[sink] == 0), 0, jnp.maximum(room, 0))
    moved = jax.random.randint(jax.random.fold_in(own, 4), (number_of // 2,), 0, 1 << 20) % (room + 1)
    tallies = tallies.at[donor].add(-moved).at[sink].add(moved)
    labels = jnp.searchsorted(jnp.cumsum(tallies), jnp.arange(rows * top), side="right").astype(jnp.int32)
    table = labels.reshape(top, rows).T
    table = table[jax.random.permutation(jax.random.fold_in(own, 1), rows)]
    offset_by = jax.random.randint(jax.random.fold_in(own, 2), (rows, 1), 0, top)
    return jnp.take_along_axis(table, (jnp.arange(top)[None, :] + offset_by) % top, axis=1)


def portions_of(number_of, total, reach, skew, full):
    weights = [(1 << 20) // math.isqrt(rank ** skew) + 1 for rank in range(1, number_of + 1)]
    largest = reach if full else min(reach, max(-(-total // number_of), total * weights[0] // sum(weights)))
    least = 1 if total - largest >= number_of - 1 else 0
    holding, rest = [largest] + [least] * (number_of - 1), total - largest - least * (number_of - 1)
    while rest > 0:
        candidates = [i for i in range(1, number_of) if holding[i] < largest] or [i for i in range(1, number_of) if holding[i] < reach]
        pool, budget = sum([weights[i] for i in candidates]), rest
        for i in candidates:
            more = min(reach - holding[i], max(1, budget * weights[i] // pool), rest)
            holding[i] = holding[i] + more
            rest = rest - more
    return np.array(holding)


def normal_values(stream_key, dims, width, reach, shards=(), held_as=jnp.bfloat16):
    entries = jax.random.normal(stream_key, dims, jnp.float32) * width
    if len(shards) > 0:
        entries = levels(stream_key, dims, shards, -0.22, 0.18) * entries
    return jnp.clip(entries, min=-reach, max=reach).astype(held_as)


def setup_inputs(seed: int = 0) -> dict:
    seeds = jax.random.split(jax.random.key(seed), 7)
    tokens = draw_tokens(jax.random.fold_in(seeds[6], 71), 0)
    expert_ids_keys = jax.random.split(jax.random.fold_in(seeds[1], 1), TOKENS // TOK_DEV)
    expert_ids_turns = jax.random.permutation(jax.random.fold_in(seeds[1], 3), TOKENS // TOK_DEV)
    expert_ids = jax.vmap(lambda own, number: routed_block(jax.random.fold_in(seeds[1], 2), own, number, TOK_DEV, EXPERTS, 1, CAP, 2))(expert_ids_keys, expert_ids_turns).reshape((TOKENS, 1))
    gate_prob = jnp.clip(0.25 + 0.75 * jax.random.uniform(seeds[2], (TOKENS,), jnp.float32) ** levels(seeds[2], (TOKENS,), ((0, 128),), -0.2, 0.2), 0.25, 1.0)
    norm_gain = jnp.clip(1.0 + 0.18 * jax.random.normal(seeds[3], (D,), jnp.float32), 0.1, 1.9)
    weight_in = normal_values(seeds[4], (EXPERTS, D, FF), D ** -0.5, 0.1875, ((0, 128),))
    weight_out = normal_values(seeds[5], (EXPERTS, FF, D), FF ** -0.5, 0.09375, ((0, 128),))
    return {"tokens": tokens, "expert_ids": expert_ids, "gate_prob": gate_prob, "norm_gain": norm_gain, "weight_in": weight_in, "weight_out": weight_out}


def slot_rank(block_ids):
    count = block_ids.shape[0]
    same = block_ids[:, None] == block_ids[None, :]
    earlier = jnp.arange(count, dtype=jnp.int32)[None, :] < jnp.arange(count, dtype=jnp.int32)[:, None]
    return lax.optimization_barrier(jnp.sum((same & earlier).astype(jnp.int32), axis=1)).astype(jnp.int32)

def expert_ffn(pieces):
    slab, first, second = pieces
    hidden = jnp.maximum(jnp.dot(slab, first, preferred_element_type=jnp.float32), 0.0).astype(jnp.bfloat16)
    return jnp.dot(hidden, second, preferred_element_type=jnp.float32).astype(jnp.bfloat16)

def reference(tokens, expert_ids, gate_prob, norm_gain, weight_in, weight_out):
    flat_ids = expert_ids[:, 0].astype(jnp.int32)
    within = jax.vmap(slot_rank)(flat_ids.reshape(DEVICES, TOK_DEV)).reshape(-1)
    source = (jnp.arange(TOKENS, dtype=jnp.int32) // TOK_DEV).astype(jnp.int32)
    placed = ((flat_ids * DEVICES + source) * CAP + within).astype(jnp.int32)
    wide = tokens.astype(jnp.float32)
    scale = lax.rsqrt(lax.optimization_barrier(jnp.mean(wide * wide, axis=1, keepdims=True)) + 1e-06)
    normed = (wide * scale * norm_gain[None, :]).astype(jnp.bfloat16)
    slots = jnp.zeros((EXPERTS * DEVICES * CAP, D), jnp.bfloat16).at[placed].set(normed)
    slots = slots.reshape(EXPERTS, DEVICES * CAP, D)
    answers = lax.map(expert_ffn, (slots, weight_in, weight_out))
    back = answers.reshape(EXPERTS * DEVICES * CAP, D)[placed]
    mixed = (wide + gate_prob[:, None] * back.astype(jnp.float32)).astype(jnp.bfloat16)
    routed = lax.optimization_barrier(jnp.sum((flat_ids[:, None] == jnp.arange(EXPERTS, dtype=jnp.int32)[None, :]).astype(jnp.int32), axis=0))
    return (mixed, routed)
```

```python
import functools

import jax
import jax.numpy as jnp
from jax import lax
from jax.experimental import pallas as pl
from jax.experimental.pallas import tpu as pltpu
from jax.sharding import PartitionSpec as P

ROW_COL = ("row", "col")
MESH = pl.DeviceIdType.MESH
TOK = 512
D = 1024
FF = 4096
CAP = 8
PEERS = 128
CHUNKS = 4
GROUP = PEERS // CHUNKS
ROWS = GROUP * CAP
SLOTS = PEERS * CAP
EMPTY = 1024.0
FF_TILE = 512
D_TILE = 256


def place():
    r = lax.axis_index("row")
    c = lax.axis_index("col")
    return lax.div(r, 2), lax.rem(r, 2), lax.div(c, 4), lax.rem(c, 4)


def peer(spot, chunk, i, sign):
    x, core, y, z = spot
    dx, dy, dc = lax.div(i, 8), lax.rem(lax.div(i, 2), 4), lax.rem(i, 2)
    dz = lax.rem(chunk + 8 - dx - dy, 4)
    if sign < 0:
        dx, dy, dz = 4 - dx, 4 - dy, 4 - dz
    row = lax.rem(x + dx, 4) * 2 + lax.rem(core + dc, 2)
    col = lax.rem(y + dy, 4) * 4 + lax.rem(z + dz, 4)
    return row, col


def kernel(
    tok_ref,
    ids_ref,
    gate_ref,
    gain_ref,
    w1_hbm,
    w2_hbm,
    out_ref,
    routed_ref,
    w1,
    w2,
    normed,
    slot_cols,
    outgoing,
    arrived,
    answers,
    returned,
    hidden,
    total,
    w_sem,
    send_out,
    recv_out,
    send_back,
    recv_back,
):
    spot = place()
    x, core, y, z = spot
    load1 = pltpu.make_async_copy(w1_hbm.at[0], w1, w_sem.at[0])
    load2 = pltpu.make_async_copy(w2_hbm.at[0], w2, w_sem.at[1])
    load1.start()
    load2.start()
    barrier = pltpu.get_barrier_semaphore()
    for chunk in range(CHUNKS):

        def greet(i, carry, chunk=chunk):
            pl.semaphore_signal(barrier, inc=1, device_id=peer(spot, chunk, i, 1), device_id_type=MESH)
            return carry

        lax.fori_loop(1 if chunk == 0 else 0, GROUP, greet, 0)

    ids_row = ids_ref[...]
    ids_cols = jnp.broadcast_to(ids_row, (128, TOK)).T
    parts = []
    for j in range(TOK // 128):
        mine = ids_row[:, j * 128 : (j + 1) * 128]
        t = lax.broadcasted_iota(jnp.int32, (TOK, 128), 1) + j * 128
        before = lax.broadcasted_iota(jnp.int32, (TOK, 128), 0) < t
        hit = jnp.where((ids_cols == mine) & before, 1.0, 0.0)
        parts.append(jnp.sum(hit, axis=0, keepdims=True))
    within = jnp.concatenate(parts, axis=1).astype(jnp.int32)
    dx = ((ids_row >> 5) - x) & 3
    dc = ((ids_row >> 4) - core) & 1
    dy = ((ids_row >> 2) - y) & 3
    dz = (ids_row - z) & 3
    order = ((dx + dy + dz) & 3) * GROUP + dx * 8 + dy * 2 + dc
    slot_row = order * CAP + within
    slot_cols[...] = jnp.broadcast_to(slot_row, (128, TOK)).T

    for b in range(TOK // 128):
        rows = pl.ds(b * 128, 128)
        wide = tok_ref[rows, :].astype(jnp.float32)
        scale = lax.rsqrt(jnp.mean(wide * wide, axis=1, keepdims=True) + 1e-06)
        normed[rows, :] = (wide * scale * gain_ref[...]).astype(jnp.bfloat16)

    ones = jnp.ones((TOK, 128), jnp.bfloat16)
    for chunk in range(CHUNKS):
        base = chunk * ROWS
        place_at = lax.broadcasted_iota(jnp.int32, (ROWS, TOK), 0) + base
        table = jnp.where(slot_row == place_at, 1.0, 0.0).astype(jnp.bfloat16)
        filled = jnp.dot(table, ones, preferred_element_type=jnp.float32)
        values = jnp.dot(table, normed[...], preferred_element_type=jnp.float32)
        first_lane = lax.broadcasted_iota(jnp.int32, (ROWS, 128), 1) == 0
        head = jnp.where(first_lane & (filled == 0.0), EMPTY, values[:, :128])
        group = pl.ds(chunk * GROUP, GROUP)
        outgoing[group, :, :128] = head.astype(jnp.bfloat16).reshape(GROUP, CAP, 128)
        outgoing[group, :, 128:] = values[:, 128:].astype(jnp.bfloat16).reshape(GROUP, CAP, D - 128)
        if chunk == 0:
            pl.semaphore_wait(barrier, PEERS - 1)

        def send(i, carry, chunk=chunk):
            k = chunk * GROUP + i
            pltpu.make_async_remote_copy(
                src_ref=outgoing.at[k],
                dst_ref=arrived.at[k],
                send_sem=send_out.at[chunk],
                recv_sem=recv_out.at[chunk],
                device_id=peer(spot, chunk, i, 1),
                device_id_type=MESH,
            ).start()
            return carry

        lax.fori_loop(1 if chunk == 0 else 0, GROUP, send, 0)
    arrived[0] = outgoing[0]

    load1.wait()
    load2.wait()
    seen = jnp.zeros((1, 128), jnp.float32)
    for chunk in range(CHUNKS):
        skip = 1 if chunk == 0 else 0
        moved = pl.ds(chunk * GROUP + skip, GROUP - skip)
        pltpu.make_async_copy(outgoing.at[moved], arrived.at[moved], recv_out.at[chunk]).wait()
        group = pl.ds(chunk * GROUP, GROUP)
        head = arrived[group, :, :128].astype(jnp.float32).reshape(ROWS, 128)
        first_lane = lax.broadcasted_iota(jnp.int32, (ROWS, 128), 1) == 0
        full = jnp.where(first_lane & (head != EMPTY), 1.0, 0.0)
        seen += jnp.sum(full, axis=0, keepdims=True)
        block = arrived[group].reshape(ROWS, D)

        def up(j, carry, block=block):
            cols = pl.ds(pl.multiple_of(j * FF_TILE, FF_TILE), FF_TILE)
            h = jnp.dot(block, w1[:, cols], preferred_element_type=jnp.float32)
            hidden[:, cols] = jnp.maximum(h, 0.0).astype(jnp.bfloat16)
            return carry

        lax.fori_loop(0, FF // FF_TILE, up, 0)

        def down(j, carry, chunk=chunk):
            cols = pl.ds(pl.multiple_of(j * D_TILE, D_TILE), D_TILE)
            a = jnp.dot(hidden[...], w2[:, cols], preferred_element_type=jnp.float32)
            answers[pl.ds(chunk * GROUP, GROUP), :, cols] = a.astype(jnp.bfloat16).reshape(GROUP, CAP, D_TILE)
            return carry

        lax.fori_loop(0, D // D_TILE, down, 0)

        def reply(i, carry, chunk=chunk):
            k = chunk * GROUP + i
            pltpu.make_async_remote_copy(
                src_ref=answers.at[k],
                dst_ref=returned.at[k],
                send_sem=send_back.at[chunk],
                recv_sem=recv_back.at[chunk],
                device_id=peer(spot, chunk, i, -1),
                device_id_type=MESH,
            ).start()
            return carry

        lax.fori_loop(skip, GROUP, reply, 0)
        if chunk == 0:
            returned[0] = answers[0]
    routed_ref[0] = jnp.sum(seen).astype(jnp.int32)

    gate_cols = jnp.broadcast_to(gate_ref[...], (128, TOK)).T
    for chunk in range(CHUNKS):
        skip = 1 if chunk == 0 else 0
        moved = pl.ds(chunk * GROUP + skip, GROUP - skip)
        picks = []
        for j in range(ROWS // 128):
            lane = lax.broadcasted_iota(jnp.int32, (TOK, 128), 1) + (chunk * ROWS + j * 128)
            picks.append(jnp.where(slot_cols[...] == lane, 1.0, 0.0).astype(jnp.bfloat16))
        pick = jnp.concatenate(picks, axis=1)
        pltpu.make_async_copy(answers.at[moved], returned.at[moved], recv_back.at[chunk]).wait()
        block = returned[pl.ds(chunk * GROUP, GROUP)].reshape(ROWS, D)
        back = jnp.dot(pick, block, preferred_element_type=jnp.float32)
        if chunk == 0:
            total[...] = back
        elif chunk < CHUNKS - 1:
            total[...] += back
        else:
            for j in range(D // 128):
                cols = slice(j * 128, (j + 1) * 128)
                got = total[:, cols] + back[:, cols]
                out_ref[:, cols] = (tok_ref[:, cols].astype(jnp.float32) + gate_cols * got).astype(jnp.bfloat16)
    for chunk in range(CHUNKS):
        skip = 1 if chunk == 0 else 0
        moved = pl.ds(chunk * GROUP + skip, GROUP - skip)
        pltpu.make_async_copy(outgoing.at[moved], arrived.at[moved], send_out.at[chunk]).wait()
        pltpu.make_async_copy(answers.at[moved], returned.at[moved], send_back.at[chunk]).wait()


def on_device(tokens, expert_ids, gate_prob, norm_gain, weight_in, weight_out):
    vmem = pl.BlockSpec(memory_space=pltpu.VMEM)
    hbm = pl.BlockSpec(memory_space=pl.ANY)
    slab = pltpu.VMEM((PEERS, CAP, D), jnp.bfloat16)
    mixed, routed = pl.pallas_call(
        kernel,
        out_shape=(
            jax.ShapeDtypeStruct((TOK, D), jnp.bfloat16),
            jax.ShapeDtypeStruct((1,), jnp.int32),
        ),
        in_specs=[vmem, vmem, vmem, vmem, hbm, hbm],
        out_specs=(vmem, pl.BlockSpec(memory_space=pltpu.SMEM)),
        scratch_shapes=[
            pltpu.VMEM((D, FF), jnp.bfloat16),
            pltpu.VMEM((FF, D), jnp.bfloat16),
            pltpu.VMEM((TOK, D), jnp.bfloat16),
            pltpu.VMEM((TOK, 128), jnp.int32),
            slab,
            slab,
            slab,
            slab,
            pltpu.VMEM((ROWS, FF), jnp.bfloat16),
            pltpu.VMEM((TOK, D), jnp.float32),
            pltpu.SemaphoreType.DMA((2,)),
            pltpu.SemaphoreType.DMA((CHUNKS,)),
            pltpu.SemaphoreType.DMA((CHUNKS,)),
            pltpu.SemaphoreType.DMA((CHUNKS,)),
            pltpu.SemaphoreType.DMA((CHUNKS,)),
        ],
        compiler_params=pltpu.CompilerParams(
            collective_id=0, has_side_effects=True, vmem_limit_bytes=56 * 2**20
        ),
    )(
        tokens,
        expert_ids.reshape(1, TOK),
        gate_prob.reshape(1, TOK),
        norm_gain.reshape(1, D),
        weight_in,
        weight_out,
    )
    return mixed, routed


def solution(mesh):
    return jax.shard_map(
        on_device,
        mesh=mesh,
        in_specs=(
            P(ROW_COL, None),
            P(ROW_COL, None),
            P(ROW_COL),
            P(),
            P(ROW_COL, None, None),
            P(ROW_COL, None, None),
        ),
        out_specs=(P(ROW_COL, None), P(ROW_COL)),
        check_vma=False,
    )
```

```python
import jax
import jax.numpy as jnp
from jax import lax
from jax.experimental import pallas as pl
from jax.experimental.pallas import tpu as pltpu
from jax.sharding import PartitionSpec as P

ROW_COL = ("row", "col")
MESH = pl.DeviceIdType.MESH
TOK = 512
D = 1024
FF = 4096
CAP = 8
PEERS = 128
SLOTS = PEERS * CAP
CLASSES = 4
CLASS = PEERS // CLASSES
GROUPS = ((0, 32), (32, 32), (64, 32), (96, 32))
MOST = max(count for _, count in GROUPS) * CAP
EMPTY = 1024.0
FF_TILE = 512
D_TILE = 256
LANES = 128
VMEM_LIMIT = 44 * 2**20


def offset(k):
    dx, dy, dc = k // 8 % 4, k // 2 % 4, k % 2
    return dx, dy, (k // CLASS - dx - dy) % 4, dc


def hops(k):
    return sum(min(d, 4 - d) for d in offset(k)[:3])


FAR_FIRST = sorted(range(1, PEERS), key=lambda k: -hops(k))


class Place:
    def __init__(self):
        r = lax.axis_index("row")
        c = lax.axis_index("col")
        self.x, self.core = lax.div(r, 2), lax.rem(r, 2)
        self.y, self.z = lax.div(c, 4), lax.rem(c, 4)
        self.xs = [lax.rem(self.x + d, 4) * 2 for d in range(4)]
        self.cores = [lax.rem(self.core + d, 2) for d in range(2)]
        self.ys = [lax.rem(self.y + d, 4) * 4 for d in range(4)]
        self.zs = [lax.rem(self.z + d, 4) for d in range(4)]

    def peer(self, k, sign):
        dx, dy, dz, dc = offset(k)
        if sign < 0:
            dx, dy, dz = -dx % 4, -dy % 4, -dz % 4
        return self.xs[dx] + self.cores[dc], self.ys[dy] + self.zs[dz]


def group_of(k):
    return next(g for g, (first, count) in enumerate(GROUPS) if first <= k < first + count)


def moved(g):
    first, count = GROUPS[g]
    skip = 1 if first == 0 else 0
    return pl.ds(first + skip, count - skip)


def columns(row):
    return jnp.broadcast_to(row, (LANES, TOK)).T


def kernel(
    tok_hbm,
    ids_hbm,
    gate_hbm,
    gain_hbm,
    w1_hbm,
    w2_hbm,
    out_ref,
    routed_ref,
    tok,
    ids,
    gate,
    gain,
    w1,
    w2,
    normed,
    slot_cols,
    outgoing,
    arrived,
    answers,
    returned,
    hidden,
    total,
    load_sem,
    send_out,
    recv_out,
    send_back,
    recv_back,
):
    here = Place()
    loads = [
        pltpu.make_async_copy(source, target, load_sem.at[n])
        for n, (source, target) in enumerate(
            [
                (ids_hbm, ids),
                (tok_hbm, tok),
                (gain_hbm, gain),
                (w1_hbm.at[0], w1),
                (w2_hbm.at[0], w2),
                (gate_hbm, gate),
            ]
        )
    ]
    for load in loads[:3]:
        load.start()
    barrier = pltpu.get_barrier_semaphore()
    for k in FAR_FIRST:
        pl.semaphore_signal(barrier, inc=1, device_id=here.peer(k, 1), device_id_type=MESH)
    for load in loads[3:]:
        load.start()

    loads[0].wait()
    ids_row = ids[...]
    ids_cols = columns(ids_row)
    parts = []
    for j in range(TOK // LANES):
        mine = ids_row[:, j * LANES : (j + 1) * LANES]
        t = lax.broadcasted_iota(jnp.int32, (TOK, LANES), 1) + j * LANES
        before = lax.broadcasted_iota(jnp.int32, (TOK, LANES), 0) < t
        hit = jnp.where((ids_cols == mine) & before, 1.0, 0.0)
        parts.append(jnp.sum(hit, axis=0, keepdims=True))
    within = jnp.concatenate(parts, axis=1).astype(jnp.int32)
    dx = ((ids_row >> 5) - here.x) & 3
    dc = ((ids_row >> 4) - here.core) & 1
    dy = ((ids_row >> 2) - here.y) & 3
    dz = (ids_row - here.z) & 3
    slot_row = (((dx + dy + dz) & 3) * CLASS + dx * 8 + dy * 2 + dc) * CAP + within
    slot_cols[...] = columns(slot_row)

    loads[1].wait()
    loads[2].wait()
    for b in range(TOK // LANES):
        rows = pl.ds(b * LANES, LANES)
        wide = tok[rows, :].astype(jnp.float32)
        scale = lax.rsqrt(jnp.mean(wide * wide, axis=1, keepdims=True) + 1e-06)
        normed[rows, :] = (wide * scale * gain[...]).astype(jnp.bfloat16)

    ones = jnp.ones((TOK, LANES), jnp.bfloat16)
    rows = CLASS * CAP
    for c in range(CLASSES):
        places = lax.broadcasted_iota(jnp.int32, (rows, TOK), 0) + c * rows
        table = jnp.where(slot_row == places, 1.0, 0.0).astype(jnp.bfloat16)
        filled = jnp.dot(table, ones, preferred_element_type=jnp.float32)
        values = jnp.dot(table, normed[...], preferred_element_type=jnp.float32)
        first_lane = lax.broadcasted_iota(jnp.int32, (rows, LANES), 1) == 0
        head = jnp.where(first_lane & (filled == 0.0), EMPTY, values[:, :LANES])
        part = pl.ds(c * CLASS, CLASS)
        outgoing[part, :, :LANES] = head.astype(jnp.bfloat16).reshape(CLASS, CAP, LANES)
        outgoing[part, :, LANES:] = values[:, LANES:].astype(jnp.bfloat16).reshape(CLASS, CAP, D - LANES)
        if c == 0:
            pl.semaphore_wait(barrier, PEERS - 1)
        for k in range(max(c * CLASS, 1), (c + 1) * CLASS):
            pltpu.make_async_remote_copy(
                src_ref=outgoing.at[k],
                dst_ref=arrived.at[k],
                send_sem=send_out.at[group_of(k)],
                recv_sem=recv_out.at[group_of(k)],
                device_id=here.peer(k, 1),
                device_id_type=MESH,
            ).start()
    arrived[0] = outgoing[0]

    seen = jnp.zeros((1, LANES), jnp.float32)
    for g, (first, count) in enumerate(GROUPS):
        rows = count * CAP
        if g == 0:
            loads[3].wait()
            loads[4].wait()
        pltpu.make_async_copy(outgoing.at[moved(g)], arrived.at[moved(g)], recv_out.at[g]).wait()
        part = pl.ds(first, count)
        head = arrived[part, :, :LANES].astype(jnp.float32).reshape(rows, LANES)
        first_lane = lax.broadcasted_iota(jnp.int32, (rows, LANES), 1) == 0
        seen += jnp.sum(jnp.where(first_lane & (head != EMPTY), 1.0, 0.0), axis=0, keepdims=True)
        block = arrived[part].reshape(rows, D)

        def up(j, carry, block=block, rows=rows):
            cols = pl.ds(pl.multiple_of(j * FF_TILE, FF_TILE), FF_TILE)
            h = jnp.dot(block, w1[:, cols], preferred_element_type=jnp.float32)
            hidden[:rows, cols] = jnp.maximum(h, 0.0).astype(jnp.bfloat16)
            return carry

        lax.fori_loop(0, FF // FF_TILE, up, 0)

        def down(j, carry, part=part, count=count, rows=rows):
            cols = pl.ds(pl.multiple_of(j * D_TILE, D_TILE), D_TILE)
            a = jnp.dot(hidden[:rows], w2[:, cols], preferred_element_type=jnp.float32)
            answers[part, :, cols] = a.astype(jnp.bfloat16).reshape(count, CAP, D_TILE)
            return carry

        lax.fori_loop(0, D // D_TILE, down, 0)
        for k in range(max(first, 1), first + count):
            pltpu.make_async_remote_copy(
                src_ref=answers.at[k],
                dst_ref=returned.at[k],
                send_sem=send_back.at[g],
                recv_sem=recv_back.at[g],
                device_id=here.peer(k, -1),
                device_id_type=MESH,
            ).start()
        if g == 0:
            returned[0] = answers[0]
    routed_ref[0] = jnp.sum(seen).astype(jnp.int32)

    loads[5].wait()
    gate_cols = columns(gate[...])
    for g, (first, count) in enumerate(GROUPS):
        picks = []
        for j in range(count * CAP // LANES):
            lane = lax.broadcasted_iota(jnp.int32, (TOK, LANES), 1) + (first * CAP + j * LANES)
            picks.append(jnp.where(slot_cols[...] == lane, 1.0, 0.0).astype(jnp.bfloat16))
        pick = jnp.concatenate(picks, axis=1)
        pltpu.make_async_copy(answers.at[moved(g)], returned.at[moved(g)], recv_back.at[g]).wait()
        block = returned[pl.ds(first, count)].reshape(count * CAP, D)
        back = jnp.dot(pick, block, preferred_element_type=jnp.float32)
        if g == 0:
            total[...] = back
        elif g < len(GROUPS) - 1:
            total[...] += back
        else:
            for j in range(D // LANES):
                cols = slice(j * LANES, (j + 1) * LANES)
                got = gate_cols * (total[:, cols] + back[:, cols])
                out_ref[:, cols] = (tok[:, cols].astype(jnp.float32) + got).astype(jnp.bfloat16)
    for g in range(len(GROUPS)):
        pltpu.make_async_copy(outgoing.at[moved(g)], arrived.at[moved(g)], send_out.at[g]).wait()
        pltpu.make_async_copy(answers.at[moved(g)], returned.at[moved(g)], send_back.at[g]).wait()


def put_out(mixed, count, mixed_out, count_out, sem):
    first = pltpu.make_async_copy(mixed, mixed_out, sem.at[0])
    second = pltpu.make_async_copy(count, count_out, sem.at[1])
    first.start()
    second.start()
    first.wait()
    second.wait()


def on_device(tokens, expert_ids, gate_prob, norm_gain, weight_in, weight_out):
    vmem = pl.BlockSpec(memory_space=pltpu.VMEM)
    smem = pl.BlockSpec(memory_space=pltpu.SMEM)
    hbm = pl.BlockSpec(memory_space=pltpu.HBM)
    outs = (jax.ShapeDtypeStruct((TOK, D), jnp.bfloat16), jax.ShapeDtypeStruct((1,), jnp.int32))
    slab = pltpu.VMEM((PEERS, CAP, D), jnp.bfloat16)
    sems = pltpu.SemaphoreType.DMA((len(GROUPS),))
    mixed, routed = pl.pallas_call(
        kernel,
        out_shape=(pltpu.VMEM((TOK, D), jnp.bfloat16), pltpu.HBM((1,), jnp.int32)),
        in_specs=[hbm] * 6,
        out_specs=(vmem, smem),
        scratch_shapes=[
            pltpu.VMEM((TOK, D), jnp.bfloat16),
            pltpu.VMEM((1, TOK), jnp.int32),
            pltpu.VMEM((1, TOK), jnp.float32),
            pltpu.VMEM((1, D), jnp.float32),
            pltpu.VMEM((D, FF), jnp.bfloat16),
            pltpu.VMEM((FF, D), jnp.bfloat16),
            pltpu.VMEM((TOK, D), jnp.bfloat16),
            pltpu.VMEM((TOK, LANES), jnp.int32),
            slab,
            slab,
            slab,
            slab,
            pltpu.VMEM((MOST, FF), jnp.bfloat16),
            pltpu.VMEM((TOK, D), jnp.float32),
            pltpu.SemaphoreType.DMA((6,)),
            sems,
            sems,
            sems,
            sems,
        ],
        compiler_params=pltpu.CompilerParams(
            collective_id=0, has_side_effects=True, vmem_limit_bytes=VMEM_LIMIT
        ),
    )(
        *(
            pltpu.with_memory_space_constraint(a, pltpu.HBM)
            for a in (
                tokens,
                expert_ids.reshape(1, TOK),
                gate_prob.reshape(1, TOK),
                norm_gain.reshape(1, D),
                weight_in,
                weight_out,
            )
        )
    )
    return pl.pallas_call(
        put_out,
        out_shape=outs,
        in_specs=[vmem, hbm],
        out_specs=(hbm, hbm),
        scratch_shapes=[pltpu.SemaphoreType.DMA((2,))],
        compiler_params=pltpu.CompilerParams(vmem_limit_bytes=8 * 2**20),
    )(mixed, routed)


def solution(mesh):
    return jax.shard_map(
        on_device,
        mesh=mesh,
        in_specs=(
            P(ROW_COL, None),
            P(ROW_COL, None),
            P(ROW_COL),
            P(),
            P(ROW_COL, None, None),
            P(ROW_COL, None, None),
        ),
        out_specs=(P(ROW_COL, None), P(ROW_COL)),
        check_vma=False,
    )
```

```python
import jax
import jax.numpy as jnp
from jax import lax
from jax.experimental import pallas as pl
from jax.experimental.pallas import tpu as pltpu
from jax.sharding import PartitionSpec as P

ROW_COL = ("row", "col")
MESH = pl.DeviceIdType.MESH
TOK = 512
D = 1024
FF = 4096
CAP = 8
PEERS = 128
SLOTS = PEERS * CAP
CLASS = PEERS // 4
GROUPS = ((0, 16), (16, 32), (48, 32), (80, 32), (112, 16))
PIECES = ((0, 16), (16, 16), (32, 32), (64, 32), (96, 32))
MOST = max(count for _, count in GROUPS) * CAP
EMPTY = 1024.0
FF_TILE = 512
D_TILE = 256
LANES = 128
OUT_PIECES = 4
VMEM_LIMIT = 44 * 2**20


def offset(k):
    dx, dc = k // 4 % 4, k % 2
    dy = (dx - k // 16 % 2 * 2 - k // 2 % 2) % 4
    return dx, dy, (k // CLASS - dx - dy) % 4, dc


def hops(k):
    return sum(min(d, 4 - d) for d in offset(k)[:3])


FAR_FIRST = sorted(range(1, PEERS), key=lambda k: -hops(k))


class Place:
    def __init__(self):
        r = lax.axis_index("row")
        c = lax.axis_index("col")
        self.x, self.core = lax.div(r, 2), lax.rem(r, 2)
        self.y, self.z = lax.div(c, 4), lax.rem(c, 4)
        self.xs = [lax.rem(self.x + d, 4) * 2 for d in range(4)]
        self.cores = [lax.rem(self.core + d, 2) for d in range(2)]
        self.ys = [lax.rem(self.y + d, 4) * 4 for d in range(4)]
        self.zs = [lax.rem(self.z + d, 4) for d in range(4)]

    def peer(self, k, sign):
        dx, dy, dz, dc = offset(k)
        if sign < 0:
            dx, dy, dz = -dx % 4, -dy % 4, -dz % 4
        return self.xs[dx] + self.cores[dc], self.ys[dy] + self.zs[dz]


def group_of(k):
    return next(g for g, (first, count) in enumerate(GROUPS) if first <= k < first + count)


def moved(g):
    first, count = GROUPS[g]
    skip = 1 if first == 0 else 0
    return pl.ds(first + skip, count - skip)


def columns(row):
    return jnp.broadcast_to(row, (LANES, TOK)).T


def kernel(
    tok_hbm,
    ids_hbm,
    gate_hbm,
    gain_hbm,
    w1_hbm,
    w2_hbm,
    out_ref,
    routed_ref,
    tok,
    ids,
    gate,
    gain,
    w1,
    w2,
    normed,
    slot_cols,
    outgoing,
    arrived,
    answers,
    returned,
    hidden,
    total,
    load_sem,
    send_out,
    recv_out,
    send_back,
    recv_back,
):
    here = Place()
    loads = [
        pltpu.make_async_copy(source, target, load_sem.at[n])
        for n, (source, target) in enumerate(
            [
                (ids_hbm, ids),
                (tok_hbm, tok),
                (gain_hbm, gain),
                (w1_hbm.at[0], w1),
                (w2_hbm.at[0], w2),
                (gate_hbm, gate),
            ]
        )
    ]
    for load in loads[:3]:
        load.start()
    barrier = pltpu.get_barrier_semaphore()
    for k in FAR_FIRST:
        pl.semaphore_signal(barrier, inc=1, device_id=here.peer(k, 1), device_id_type=MESH)
    for load in loads[3:]:
        load.start()

    loads[0].wait()
    ids_row = ids[...]
    ids_cols = columns(ids_row)
    parts = []
    for j in range(TOK // LANES):
        mine = ids_row[:, j * LANES : (j + 1) * LANES]
        t = lax.broadcasted_iota(jnp.int32, (TOK, LANES), 1) + j * LANES
        before = lax.broadcasted_iota(jnp.int32, (TOK, LANES), 0) < t
        hit = jnp.where((ids_cols == mine) & before, 1.0, 0.0)
        parts.append(jnp.sum(hit, axis=0, keepdims=True))
    within = jnp.concatenate(parts, axis=1).astype(jnp.int32)
    dx = ((ids_row >> 5) - here.x) & 3
    dc = ((ids_row >> 4) - here.core) & 1
    dy = ((ids_row >> 2) - here.y) & 3
    dz = (ids_row - here.z) & 3
    turn = (dx - dy) & 3
    inside = (turn >> 1) * 16 + dx * 4 + (turn & 1) * 2 + dc
    slot_row = (((dx + dy + dz) & 3) * CLASS + inside) * CAP + within
    slot_cols[...] = columns(slot_row)

    loads[1].wait()
    loads[2].wait()
    for b in range(TOK // LANES):
        rows = pl.ds(b * LANES, LANES)
        wide = tok[rows, :].astype(jnp.float32)
        scale = lax.rsqrt(jnp.mean(wide * wide, axis=1, keepdims=True) + 1e-06)
        normed[rows, :] = (wide * scale * gain[...]).astype(jnp.bfloat16)

    ones = jnp.ones((TOK, LANES), jnp.bfloat16)
    for first, count in PIECES:
        rows = count * CAP
        places = lax.broadcasted_iota(jnp.int32, (rows, TOK), 0) + first * CAP
        table = jnp.where(slot_row == places, 1.0, 0.0).astype(jnp.bfloat16)
        filled = jnp.dot(table, ones, preferred_element_type=jnp.float32)
        values = jnp.dot(table, normed[...], preferred_element_type=jnp.float32)
        first_lane = lax.broadcasted_iota(jnp.int32, (rows, LANES), 1) == 0
        head = jnp.where(first_lane & (filled == 0.0), EMPTY, values[:, :LANES])
        part = pl.ds(first, count)
        outgoing[part, :, :LANES] = head.astype(jnp.bfloat16).reshape(count, CAP, LANES)
        outgoing[part, :, LANES:] = values[:, LANES:].astype(jnp.bfloat16).reshape(count, CAP, D - LANES)
        if first == 0:
            pl.semaphore_wait(barrier, PEERS - 1)
        for k in range(max(first, 1), first + count):
            pltpu.make_async_remote_copy(
                src_ref=outgoing.at[k],
                dst_ref=arrived.at[k],
                send_sem=send_out.at[group_of(k)],
                recv_sem=recv_out.at[group_of(k)],
                device_id=here.peer(k, 1),
                device_id_type=MESH,
            ).start()
    arrived[0] = outgoing[0]

    seen = jnp.zeros((1, LANES), jnp.float32)
    for g, (first, count) in enumerate(GROUPS):
        rows = count * CAP
        if g == 0:
            loads[3].wait()
            loads[4].wait()
        pltpu.make_async_copy(outgoing.at[moved(g)], arrived.at[moved(g)], recv_out.at[g]).wait()
        part = pl.ds(first, count)
        head = arrived[part, :, :LANES].astype(jnp.float32).reshape(rows, LANES)
        first_lane = lax.broadcasted_iota(jnp.int32, (rows, LANES), 1) == 0
        seen += jnp.sum(jnp.where(first_lane & (head != EMPTY), 1.0, 0.0), axis=0, keepdims=True)
        block = arrived[part].reshape(rows, D)

        def up(j, carry, block=block, rows=rows):
            cols = pl.ds(pl.multiple_of(j * FF_TILE, FF_TILE), FF_TILE)
            h = jnp.dot(block, w1[:, cols], preferred_element_type=jnp.float32)
            hidden[:rows, cols] = jnp.maximum(h, 0.0).astype(jnp.bfloat16)
            return carry

        lax.fori_loop(0, FF // FF_TILE, up, 0)

        def down(j, carry, part=part, count=count, rows=rows):
            cols = pl.ds(pl.multiple_of(j * D_TILE, D_TILE), D_TILE)
            a = jnp.dot(hidden[:rows], w2[:, cols], preferred_element_type=jnp.float32)
            answers[part, :, cols] = a.astype(jnp.bfloat16).reshape(count, CAP, D_TILE)
            return carry

        lax.fori_loop(0, D // D_TILE, down, 0)
        for k in range(max(first, 1), first + count):
            pltpu.make_async_remote_copy(
                src_ref=answers.at[k],
                dst_ref=returned.at[k],
                send_sem=send_back.at[g],
                recv_sem=recv_back.at[g],
                device_id=here.peer(k, -1),
                device_id_type=MESH,
            ).start()
        if g == 0:
            returned[0] = answers[0]
    routed_ref[0] = jnp.sum(seen).astype(jnp.int32)

    loads[5].wait()
    gate_cols = columns(gate[...])
    for g, (first, count) in enumerate(GROUPS):
        picks = []
        for j in range(count * CAP // LANES):
            lane = lax.broadcasted_iota(jnp.int32, (TOK, LANES), 1) + (first * CAP + j * LANES)
            picks.append(jnp.where(slot_cols[...] == lane, 1.0, 0.0).astype(jnp.bfloat16))
        pick = jnp.concatenate(picks, axis=1)
        pltpu.make_async_copy(answers.at[moved(g)], returned.at[moved(g)], recv_back.at[g]).wait()
        block = returned[pl.ds(first, count)].reshape(count * CAP, D)
        back = jnp.dot(pick, block, preferred_element_type=jnp.float32)
        if g == 0:
            total[...] = back
        elif g < len(GROUPS) - 2:
            total[...] += back
        else:
            for j in range(D // LANES):
                cols = slice(j * LANES, (j + 1) * LANES)
                if g < len(GROUPS) - 1:
                    got = gate_cols * (total[:, cols] + back[:, cols])
                    total[:, cols] = tok[:, cols].astype(jnp.float32) + got
                else:
                    out_ref[:, cols] = (total[:, cols] + gate_cols * back[:, cols]).astype(jnp.bfloat16)
    for g in range(len(GROUPS)):
        pltpu.make_async_copy(outgoing.at[moved(g)], arrived.at[moved(g)], send_out.at[g]).wait()
        pltpu.make_async_copy(answers.at[moved(g)], returned.at[moved(g)], send_back.at[g]).wait()


def put_out(mixed, count, mixed_out, count_out, sem):
    step = TOK // OUT_PIECES
    copies = [pltpu.make_async_copy(count, count_out, sem.at[OUT_PIECES])]
    for n in range(OUT_PIECES):
        rows = pl.ds(n * step, step)
        copies.append(pltpu.make_async_copy(mixed.at[rows], mixed_out.at[rows], sem.at[n]))
    for copy in copies:
        copy.start()
    for copy in copies:
        copy.wait()


def on_device(tokens, expert_ids, gate_prob, norm_gain, weight_in, weight_out):
    vmem = pl.BlockSpec(memory_space=pltpu.VMEM)
    smem = pl.BlockSpec(memory_space=pltpu.SMEM)
    hbm = pl.BlockSpec(memory_space=pltpu.HBM)
    outs = (jax.ShapeDtypeStruct((TOK, D), jnp.bfloat16), jax.ShapeDtypeStruct((1,), jnp.int32))
    slab = pltpu.VMEM((PEERS, CAP, D), jnp.bfloat16)
    sems = pltpu.SemaphoreType.DMA((len(GROUPS),))
    mixed, routed = pl.pallas_call(
        kernel,
        out_shape=(pltpu.VMEM((TOK, D), jnp.bfloat16), pltpu.SMEM((1,), jnp.int32)),
        in_specs=[hbm] * 6,
        out_specs=(vmem, smem),
        scratch_shapes=[
            pltpu.VMEM((TOK, D), jnp.bfloat16),
            pltpu.VMEM((1, TOK), jnp.int32),
            pltpu.VMEM((1, TOK), jnp.float32),
            pltpu.VMEM((1, D), jnp.float32),
            pltpu.VMEM((D, FF), jnp.bfloat16),
            pltpu.VMEM((FF, D), jnp.bfloat16),
            pltpu.VMEM((TOK, D), jnp.bfloat16),
            pltpu.VMEM((TOK, LANES), jnp.int32),
            slab,
            slab,
            slab,
            slab,
            pltpu.VMEM((MOST, FF), jnp.bfloat16),
            pltpu.VMEM((TOK, D), jnp.float32),
            pltpu.SemaphoreType.DMA((6,)),
            sems,
            sems,
            sems,
            sems,
        ],
        compiler_params=pltpu.CompilerParams(
            collective_id=0, has_side_effects=True, vmem_limit_bytes=VMEM_LIMIT
        ),
    )(
        *(
            pltpu.with_memory_space_constraint(a, pltpu.HBM)
            for a in (
                tokens,
                expert_ids.reshape(1, TOK),
                gate_prob.reshape(1, TOK),
                norm_gain.reshape(1, D),
                weight_in,
                weight_out,
            )
        )
    )
    return pl.pallas_call(
        put_out,
        out_shape=outs,
        in_specs=[vmem, smem],
        out_specs=(hbm, hbm),
        scratch_shapes=[pltpu.SemaphoreType.DMA((OUT_PIECES + 1,))],
        compiler_params=pltpu.CompilerParams(vmem_limit_bytes=8 * 2**20),
    )(mixed, routed)


def solution(mesh):
    return jax.shard_map(
        on_device,
        mesh=mesh,
        in_specs=(
            P(ROW_COL, None),
            P(ROW_COL, None),
            P(ROW_COL),
            P(),
            P(ROW_COL, None, None),
            P(ROW_COL, None, None),
        ),
        out_specs=(P(ROW_COL, None), P(ROW_COL)),
        check_vma=False,
    )
```

```python
import jax
import jax.numpy as jnp
from jax import lax
from jax.experimental import pallas as pl
from jax.experimental.pallas import tpu as pltpu
from jax.sharding import PartitionSpec as P

ROW_COL = ("row", "col")
MESH = pl.DeviceIdType.MESH
TOK = 512
D = 1024
FF = 4096
CAP = 8
PEERS = 128
SLOTS = PEERS * CAP
CLASS = PEERS // 4
GROUPS = ((0, 16), (16, 32), (48, 32), (80, 32), (112, 16))
PIECES = ((0, 16), (16, 16), (32, 32), (64, 32), (96, 32))
MOST = max(count for _, count in GROUPS) * CAP
LAST = GROUPS[-1][1] * CAP
EMPTY = 1024.0
FF_TILE = 512
D_TILE = 256
LANES = 128
OUT_PIECES = 4
VMEM_LIMIT = 44 * 2**20


def offset(k):
    dx, dc = k // 4 % 4, k % 2
    dy = (dx - k // 16 % 2 * 2 - k // 2 % 2) % 4
    return dx, dy, (k // CLASS - dx - dy) % 4, dc


def hops(k):
    return sum(min(d, 4 - d) for d in offset(k)[:3])


FAR_FIRST = sorted(range(1, PEERS), key=lambda k: -hops(k))


class Place:
    def __init__(self):
        r = lax.axis_index("row")
        c = lax.axis_index("col")
        self.x, self.core = lax.div(r, 2), lax.rem(r, 2)
        self.y, self.z = lax.div(c, 4), lax.rem(c, 4)
        self.xs = [lax.rem(self.x + d, 4) * 2 for d in range(4)]
        self.cores = [lax.rem(self.core + d, 2) for d in range(2)]
        self.ys = [lax.rem(self.y + d, 4) * 4 for d in range(4)]
        self.zs = [lax.rem(self.z + d, 4) for d in range(4)]

    def peer(self, k, sign):
        dx, dy, dz, dc = offset(k)
        if sign < 0:
            dx, dy, dz = -dx % 4, -dy % 4, -dz % 4
        return self.xs[dx] + self.cores[dc], self.ys[dy] + self.zs[dz]


def group_of(k):
    return next(g for g, (first, count) in enumerate(GROUPS) if first <= k < first + count)


def moved(g):
    first, count = GROUPS[g]
    skip = 1 if first == 0 else 0
    return pl.ds(first + skip, count - skip)


def columns(row):
    return jnp.broadcast_to(row, (LANES, TOK)).T


def kernel(
    tok_hbm,
    ids_hbm,
    gate_hbm,
    gain_hbm,
    w1_hbm,
    w2_hbm,
    total,
    last,
    last_pick,
    gate_cols_ref,
    routed_ref,
    tok,
    ids,
    gate,
    gain,
    w1,
    w2,
    normed,
    slot_cols,
    outgoing,
    arrived,
    answers,
    returned,
    hidden,
    load_sem,
    send_out,
    recv_out,
    send_back,
    recv_back,
):
    here = Place()
    loads = [
        pltpu.make_async_copy(source, target, load_sem.at[n])
        for n, (source, target) in enumerate(
            [
                (ids_hbm, ids),
                (tok_hbm, tok),
                (gain_hbm, gain),
                (w1_hbm.at[0], w1),
                (w2_hbm.at[0], w2),
                (gate_hbm, gate),
            ]
        )
    ]
    for load in loads[:3]:
        load.start()
    barrier = pltpu.get_barrier_semaphore()
    for k in FAR_FIRST:
        pl.semaphore_signal(barrier, inc=1, device_id=here.peer(k, 1), device_id_type=MESH)
    for load in loads[3:]:
        load.start()

    loads[0].wait()
    ids_row = ids[...]
    ids_cols = columns(ids_row)
    parts = []
    for j in range(TOK // LANES):
        mine = ids_row[:, j * LANES : (j + 1) * LANES]
        t = lax.broadcasted_iota(jnp.int32, (TOK, LANES), 1) + j * LANES
        before = lax.broadcasted_iota(jnp.int32, (TOK, LANES), 0) < t
        hit = jnp.where((ids_cols == mine) & before, 1.0, 0.0)
        parts.append(jnp.sum(hit, axis=0, keepdims=True))
    within = jnp.concatenate(parts, axis=1).astype(jnp.int32)
    dx = ((ids_row >> 5) - here.x) & 3
    dc = ((ids_row >> 4) - here.core) & 1
    dy = ((ids_row >> 2) - here.y) & 3
    dz = (ids_row - here.z) & 3
    turn = (dx - dy) & 3
    inside = (turn >> 1) * 16 + dx * 4 + (turn & 1) * 2 + dc
    slot_row = (((dx + dy + dz) & 3) * CLASS + inside) * CAP + within
    slot_cols[...] = columns(slot_row)

    loads[1].wait()
    loads[2].wait()
    for b in range(TOK // LANES):
        rows = pl.ds(b * LANES, LANES)
        wide = tok[rows, :].astype(jnp.float32)
        scale = lax.rsqrt(jnp.mean(wide * wide, axis=1, keepdims=True) + 1e-06)
        normed[rows, :] = (wide * scale * gain[...]).astype(jnp.bfloat16)

    ones = jnp.ones((TOK, LANES), jnp.bfloat16)
    for first, count in PIECES:
        rows = count * CAP
        places = lax.broadcasted_iota(jnp.int32, (rows, TOK), 0) + first * CAP
        table = jnp.where(slot_row == places, 1.0, 0.0).astype(jnp.bfloat16)
        filled = jnp.dot(table, ones, preferred_element_type=jnp.float32)
        values = jnp.dot(table, normed[...], preferred_element_type=jnp.float32)
        first_lane = lax.broadcasted_iota(jnp.int32, (rows, LANES), 1) == 0
        head = jnp.where(first_lane & (filled == 0.0), EMPTY, values[:, :LANES])
        part = pl.ds(first, count)
        outgoing[part, :, :LANES] = head.astype(jnp.bfloat16).reshape(count, CAP, LANES)
        outgoing[part, :, LANES:] = values[:, LANES:].astype(jnp.bfloat16).reshape(count, CAP, D - LANES)
        if first == 0:
            pl.semaphore_wait(barrier, PEERS - 1)
        for k in range(max(first, 1), first + count):
            pltpu.make_async_remote_copy(
                src_ref=outgoing.at[k],
                dst_ref=arrived.at[k],
                send_sem=send_out.at[group_of(k)],
                recv_sem=recv_out.at[group_of(k)],
                device_id=here.peer(k, 1),
                device_id_type=MESH,
            ).start()
    arrived[0] = outgoing[0]

    seen = jnp.zeros((1, LANES), jnp.float32)
    for g, (first, count) in enumerate(GROUPS):
        rows = count * CAP
        if g == 0:
            loads[3].wait()
            loads[4].wait()
        pltpu.make_async_copy(outgoing.at[moved(g)], arrived.at[moved(g)], recv_out.at[g]).wait()
        part = pl.ds(first, count)
        head = arrived[part, :, :LANES].astype(jnp.float32).reshape(rows, LANES)
        first_lane = lax.broadcasted_iota(jnp.int32, (rows, LANES), 1) == 0
        seen += jnp.sum(jnp.where(first_lane & (head != EMPTY), 1.0, 0.0), axis=0, keepdims=True)
        block = arrived[part].reshape(rows, D)

        def up(j, carry, block=block, rows=rows):
            cols = pl.ds(pl.multiple_of(j * FF_TILE, FF_TILE), FF_TILE)
            h = jnp.dot(block, w1[:, cols], preferred_element_type=jnp.float32)
            hidden[:rows, cols] = jnp.maximum(h, 0.0).astype(jnp.bfloat16)
            return carry

        lax.fori_loop(0, FF // FF_TILE, up, 0)

        def down(j, carry, part=part, count=count, rows=rows):
            cols = pl.ds(pl.multiple_of(j * D_TILE, D_TILE), D_TILE)
            a = jnp.dot(hidden[:rows], w2[:, cols], preferred_element_type=jnp.float32)
            answers[part, :, cols] = a.astype(jnp.bfloat16).reshape(count, CAP, D_TILE)
            return carry

        lax.fori_loop(0, D // D_TILE, down, 0)
        for k in range(max(first, 1), first + count):
            pltpu.make_async_remote_copy(
                src_ref=answers.at[k],
                dst_ref=returned.at[k],
                send_sem=send_back.at[g],
                recv_sem=recv_back.at[g],
                device_id=here.peer(k, -1),
                device_id_type=MESH,
            ).start()
        if g == 0:
            returned[0] = answers[0]
    routed_ref[0] = jnp.sum(seen).astype(jnp.int32)

    loads[5].wait()
    gate_cols = columns(gate[...])
    for g, (first, count) in enumerate(GROUPS):
        picks = []
        for j in range(count * CAP // LANES):
            lane = lax.broadcasted_iota(jnp.int32, (TOK, LANES), 1) + (first * CAP + j * LANES)
            picks.append(jnp.where(slot_cols[...] == lane, 1.0, 0.0).astype(jnp.bfloat16))
        pick = jnp.concatenate(picks, axis=1)
        pltpu.make_async_copy(answers.at[moved(g)], returned.at[moved(g)], recv_back.at[g]).wait()
        block = returned[pl.ds(first, count)].reshape(count * CAP, D)
        if g == len(GROUPS) - 1:
            last[...] = block
            last_pick[...] = pick
            gate_cols_ref[...] = gate_cols
            continue
        back = jnp.dot(pick, block, preferred_element_type=jnp.float32)
        if g == 0:
            total[...] = back
        elif g < len(GROUPS) - 2:
            total[...] += back
        else:
            for j in range(D // LANES):
                cols = slice(j * LANES, (j + 1) * LANES)
                got = gate_cols * (total[:, cols] + back[:, cols])
                total[:, cols] = tok[:, cols].astype(jnp.float32) + got
    for g in range(len(GROUPS)):
        pltpu.make_async_copy(outgoing.at[moved(g)], arrived.at[moved(g)], send_out.at[g]).wait()
        pltpu.make_async_copy(answers.at[moved(g)], returned.at[moved(g)], send_back.at[g]).wait()


def finish(total, last, pick, gate_cols, count, mixed_out, count_out, mixed, sem):
    step = TOK // OUT_PIECES
    copies = [pltpu.make_async_copy(count, count_out, sem.at[OUT_PIECES])]
    copies[0].start()
    for n in range(OUT_PIECES):
        rows = pl.ds(n * step, step)
        back = jnp.dot(pick[rows, :], last[...], preferred_element_type=jnp.float32)
        for j in range(D // LANES):
            cols = slice(j * LANES, (j + 1) * LANES)
            mixed[rows, cols] = (total[rows, cols] + gate_cols[rows, :] * back[:, cols]).astype(jnp.bfloat16)
        copies.append(pltpu.make_async_copy(mixed.at[rows], mixed_out.at[rows], sem.at[n]))
        copies[-1].start()
    for copy in copies:
        copy.wait()


def on_device(tokens, expert_ids, gate_prob, norm_gain, weight_in, weight_out):
    vmem = pl.BlockSpec(memory_space=pltpu.VMEM)
    smem = pl.BlockSpec(memory_space=pltpu.SMEM)
    hbm = pl.BlockSpec(memory_space=pltpu.HBM)
    outs = (jax.ShapeDtypeStruct((TOK, D), jnp.bfloat16), jax.ShapeDtypeStruct((1,), jnp.int32))
    slab = pltpu.VMEM((PEERS, CAP, D), jnp.bfloat16)
    sems = pltpu.SemaphoreType.DMA((len(GROUPS),))
    *parts, routed = pl.pallas_call(
        kernel,
        out_shape=(
            pltpu.VMEM((TOK, D), jnp.float32),
            pltpu.VMEM((LAST, D), jnp.bfloat16),
            pltpu.VMEM((TOK, LAST), jnp.bfloat16),
            pltpu.VMEM((TOK, LANES), jnp.float32),
            pltpu.SMEM((1,), jnp.int32),
        ),
        in_specs=[hbm] * 6,
        out_specs=(vmem, vmem, vmem, vmem, smem),
        scratch_shapes=[
            pltpu.VMEM((TOK, D), jnp.bfloat16),
            pltpu.VMEM((1, TOK), jnp.int32),
            pltpu.VMEM((1, TOK), jnp.float32),
            pltpu.VMEM((1, D), jnp.float32),
            pltpu.VMEM((D, FF), jnp.bfloat16),
            pltpu.VMEM((FF, D), jnp.bfloat16),
            pltpu.VMEM((TOK, D), jnp.bfloat16),
            pltpu.VMEM((TOK, LANES), jnp.int32),
            slab,
            slab,
            slab,
            slab,
            pltpu.VMEM((MOST, FF), jnp.bfloat16),
            pltpu.SemaphoreType.DMA((6,)),
            sems,
            sems,
            sems,
            sems,
        ],
        compiler_params=pltpu.CompilerParams(
            collective_id=0, has_side_effects=True, vmem_limit_bytes=VMEM_LIMIT
        ),
    )(
        *(
            pltpu.with_memory_space_constraint(a, pltpu.HBM)
            for a in (
                tokens,
                expert_ids.reshape(1, TOK),
                gate_prob.reshape(1, TOK),
                norm_gain.reshape(1, D),
                weight_in,
                weight_out,
            )
        )
    )
    return pl.pallas_call(
        finish,
        out_shape=outs,
        in_specs=[vmem, vmem, vmem, vmem, smem],
        out_specs=(hbm, hbm),
        scratch_shapes=[pltpu.VMEM((TOK, D), jnp.bfloat16), pltpu.SemaphoreType.DMA((OUT_PIECES + 1,))],
        compiler_params=pltpu.CompilerParams(vmem_limit_bytes=8 * 2**20),
    )(*parts, routed)


def solution(mesh):
    return jax.shard_map(
        on_device,
        mesh=mesh,
        in_specs=(
            P(ROW_COL, None),
            P(ROW_COL, None),
            P(ROW_COL),
            P(),
            P(ROW_COL, None, None),
            P(ROW_COL, None, None),
        ),
        out_specs=(P(ROW_COL, None), P(ROW_COL)),
        check_vma=False,
    )
```

```python
import jax
import jax.numpy as jnp
from jax import lax
from jax.experimental import pallas as pl
from jax.experimental.pallas import tpu as pltpu
from jax.sharding import PartitionSpec as P

ROW_COL = ("row", "col")
MESH = pl.DeviceIdType.MESH
TOK = 512
D = 1024
FF = 4096
CAP = 8
PEERS = 128
SLOTS = PEERS * CAP
CLASS = PEERS // 4
GROUPS = ((0, 16), (16, 32), (48, 32), (80, 32), (112, 16))
PIECES = ((0, 16), (16, 16), (32, 32), (64, 32), (96, 32))
MOST = max(count for _, count in GROUPS) * CAP
LAST = GROUPS[-1][1] * CAP
EMPTY = 1024.0
FF_TILE = 512
D_TILE = 256
LANES = 128
OUT_PIECES = 4
VMEM_LIMIT = 44 * 2**20


def offset(k):
    dx, dc = k // 4 % 4, k % 2
    dy = (dx - k // 16 % 2 * 2 - k // 2 % 2) % 4
    return dx, dy, (k // CLASS - dx - dy) % 4, dc


def hops(k):
    return sum(min(d, 4 - d) for d in offset(k)[:3])


FAR_FIRST = sorted(range(1, PEERS), key=lambda k: -hops(k))


class Place:
    def __init__(self):
        r = lax.axis_index("row")
        c = lax.axis_index("col")
        self.x, self.core = lax.div(r, 2), lax.rem(r, 2)
        self.y, self.z = lax.div(c, 4), lax.rem(c, 4)
        self.xs = [lax.rem(self.x + d, 4) * 2 for d in range(4)]
        self.cores = [lax.rem(self.core + d, 2) for d in range(2)]
        self.ys = [lax.rem(self.y + d, 4) * 4 for d in range(4)]
        self.zs = [lax.rem(self.z + d, 4) for d in range(4)]

    def peer(self, k, sign):
        dx, dy, dz, dc = offset(k)
        if sign < 0:
            dx, dy, dz = -dx % 4, -dy % 4, -dz % 4
        return self.xs[dx] + self.cores[dc], self.ys[dy] + self.zs[dz]


def group_of(k):
    return next(g for g, (first, count) in enumerate(GROUPS) if first <= k < first + count)


def moved(g):
    first, count = GROUPS[g]
    skip = 1 if first == 0 else 0
    return pl.ds(first + skip, count - skip)


def columns(row):
    return jnp.broadcast_to(row, (LANES, TOK)).T


def kernel(
    tok_hbm,
    ids_hbm,
    gate_hbm,
    gain_hbm,
    w1_hbm,
    w2_hbm,
    total,
    last,
    last_pick,
    gate_cols_ref,
    routed_ref,
    tok,
    ids,
    gate,
    gain,
    w1,
    w2,
    normed,
    slot_cols,
    outgoing,
    arrived,
    answers,
    returned,
    hidden,
    load_sem,
    send_out,
    recv_out,
    send_back,
    recv_back,
):
    here = Place()
    loads = [
        pltpu.make_async_copy(source, target, load_sem.at[n])
        for n, (source, target) in enumerate(
            [
                (ids_hbm, ids),
                (tok_hbm, tok),
                (gain_hbm, gain),
                (w1_hbm.at[0], w1),
                (w2_hbm.at[0], w2),
                (gate_hbm, gate),
            ]
        )
    ]
    for load in loads[:3]:
        load.start()
    barrier = pltpu.get_barrier_semaphore()
    for k in FAR_FIRST:
        pl.semaphore_signal(barrier, inc=1, device_id=here.peer(k, 1), device_id_type=MESH)
    for load in loads[3:]:
        load.start()

    loads[0].wait()
    ids_row = ids[...]
    ids_cols = columns(ids_row)
    parts = []
    for j in range(TOK // LANES):
        mine = ids_row[:, j * LANES : (j + 1) * LANES]
        t = lax.broadcasted_iota(jnp.int32, (TOK, LANES), 1) + j * LANES
        before = lax.broadcasted_iota(jnp.int32, (TOK, LANES), 0) < t
        hit = jnp.where((ids_cols == mine) & before, 1.0, 0.0)
        parts.append(jnp.sum(hit, axis=0, keepdims=True))
    within = jnp.concatenate(parts, axis=1).astype(jnp.int32)
    dx = ((ids_row >> 5) - here.x) & 3
    dc = ((ids_row >> 4) - here.core) & 1
    dy = ((ids_row >> 2) - here.y) & 3
    dz = (ids_row - here.z) & 3
    turn = (dx - dy) & 3
    inside = (turn >> 1) * 16 + dx * 4 + (turn & 1) * 2 + dc
    slot_row = (((dx + dy + dz) & 3) * CLASS + inside) * CAP + within
    slot_cols[...] = columns(slot_row)

    loads[1].wait()
    loads[2].wait()
    for b in range(TOK // LANES):
        rows = pl.ds(b * LANES, LANES)
        wide = tok[rows, :].astype(jnp.float32)
        scale = lax.rsqrt(jnp.mean(wide * wide, axis=1, keepdims=True) + 1e-06)
        normed[rows, :] = (wide * scale * gain[...]).astype(jnp.bfloat16)

    ones = jnp.ones((TOK, LANES), jnp.bfloat16)
    for first, count in PIECES:
        rows = count * CAP
        places = lax.broadcasted_iota(jnp.int32, (rows, TOK), 0) + first * CAP
        table = jnp.where(slot_row == places, 1.0, 0.0).astype(jnp.bfloat16)
        filled = jnp.dot(table, ones, preferred_element_type=jnp.float32)
        values = jnp.dot(table, normed[...], preferred_element_type=jnp.float32)
        first_lane = lax.broadcasted_iota(jnp.int32, (rows, LANES), 1) == 0
        head = jnp.where(first_lane & (filled == 0.0), EMPTY, values[:, :LANES])
        part = pl.ds(first, count)
        outgoing[part, :, :LANES] = head.astype(jnp.bfloat16).reshape(count, CAP, LANES)
        outgoing[part, :, LANES:] = values[:, LANES:].astype(jnp.bfloat16).reshape(count, CAP, D - LANES)
        if first == 0:
            pl.semaphore_wait(barrier, PEERS - 1)
        for k in range(max(first, 1), first + count):
            pltpu.make_async_remote_copy(
                src_ref=outgoing.at[k],
                dst_ref=arrived.at[k],
                send_sem=send_out.at[group_of(k)],
                recv_sem=recv_out.at[group_of(k)],
                device_id=here.peer(k, 1),
                device_id_type=MESH,
            ).start()
    arrived[0] = outgoing[0]

    seen = jnp.zeros((1, LANES), jnp.float32)
    for g, (first, count) in enumerate(GROUPS):
        rows = count * CAP
        if g == 0:
            loads[3].wait()
            loads[4].wait()
        pltpu.make_async_copy(outgoing.at[moved(g)], arrived.at[moved(g)], recv_out.at[g]).wait()
        part = pl.ds(first, count)
        head = arrived[part, :, :LANES].astype(jnp.float32).reshape(rows, LANES)
        first_lane = lax.broadcasted_iota(jnp.int32, (rows, LANES), 1) == 0
        seen += jnp.sum(jnp.where(first_lane & (head != EMPTY), 1.0, 0.0), axis=0, keepdims=True)
        block = arrived[part].reshape(rows, D)

        def up(j, carry, block=block, rows=rows):
            cols = pl.ds(pl.multiple_of(j * FF_TILE, FF_TILE), FF_TILE)
            h = jnp.dot(block, w1[:, cols], preferred_element_type=jnp.float32)
            hidden[:rows, cols] = jnp.maximum(h, 0.0).astype(jnp.bfloat16)
            return carry

        lax.fori_loop(0, FF // FF_TILE, up, 0)

        def down(j, carry, part=part, count=count, rows=rows):
            cols = pl.ds(pl.multiple_of(j * D_TILE, D_TILE), D_TILE)
            a = jnp.dot(hidden[:rows], w2[:, cols], preferred_element_type=jnp.float32)
            answers[part, :, cols] = a.astype(jnp.bfloat16).reshape(count, CAP, D_TILE)
            return carry

        lax.fori_loop(0, D // D_TILE, down, 0)
        for k in range(max(first, 1), first + count):
            pltpu.make_async_remote_copy(
                src_ref=answers.at[k],
                dst_ref=returned.at[k],
                send_sem=send_back.at[g],
                recv_sem=recv_back.at[g],
                device_id=here.peer(k, -1),
                device_id_type=MESH,
            ).start()
        if g == 0:
            returned[0] = answers[0]
    routed_ref[0] = jnp.sum(seen).astype(jnp.int32)

    loads[5].wait()
    gate_cols = columns(gate[...])
    for g, (first, count) in enumerate(GROUPS):
        picks = []
        for j in range(count * CAP // LANES):
            lane = lax.broadcasted_iota(jnp.int32, (TOK, LANES), 1) + (first * CAP + j * LANES)
            picks.append(jnp.where(slot_cols[...] == lane, 1.0, 0.0).astype(jnp.bfloat16))
        pick = jnp.concatenate(picks, axis=1)
        if g == len(GROUPS) - 1:
            last_pick[...] = pick
            gate_cols_ref[...] = gate_cols
        pltpu.make_async_copy(answers.at[moved(g)], returned.at[moved(g)], recv_back.at[g]).wait()
        block = returned[pl.ds(first, count)].reshape(count * CAP, D)
        if g == len(GROUPS) - 1:
            last[...] = block
            continue
        back = jnp.dot(pick, block, preferred_element_type=jnp.float32)
        if g == 0:
            total[...] = back
        elif g < len(GROUPS) - 2:
            total[...] += back
        else:
            for j in range(D // LANES):
                cols = slice(j * LANES, (j + 1) * LANES)
                got = gate_cols * (total[:, cols] + back[:, cols])
                total[:, cols] = tok[:, cols].astype(jnp.float32) + got
    for g in range(len(GROUPS)):
        pltpu.make_async_copy(outgoing.at[moved(g)], arrived.at[moved(g)], send_out.at[g]).wait()
        pltpu.make_async_copy(answers.at[moved(g)], returned.at[moved(g)], send_back.at[g]).wait()


def finish(total, last, pick, gate_cols, count, mixed_out, count_out, mixed, sem):
    step = TOK // OUT_PIECES
    copies = [pltpu.make_async_copy(count, count_out, sem.at[OUT_PIECES])]
    copies[0].start()
    for n in range(OUT_PIECES):
        rows = pl.ds(n * step, step)
        back = jnp.dot(pick[rows, :], last[...], preferred_element_type=jnp.float32)
        for j in range(D // LANES):
            cols = slice(j * LANES, (j + 1) * LANES)
            mixed[rows, cols] = (total[rows, cols] + gate_cols[rows, :] * back[:, cols]).astype(jnp.bfloat16)
        copies.append(pltpu.make_async_copy(mixed.at[rows], mixed_out.at[rows], sem.at[n]))
        copies[-1].start()
    for copy in copies:
        copy.wait()


def on_device(tokens, expert_ids, gate_prob, norm_gain, weight_in, weight_out):
    vmem = pl.BlockSpec(memory_space=pltpu.VMEM)
    smem = pl.BlockSpec(memory_space=pltpu.SMEM)
    hbm = pl.BlockSpec(memory_space=pltpu.HBM)
    outs = (jax.ShapeDtypeStruct((TOK, D), jnp.bfloat16), jax.ShapeDtypeStruct((1,), jnp.int32))
    slab = pltpu.VMEM((PEERS, CAP, D), jnp.bfloat16)
    sems = pltpu.SemaphoreType.DMA((len(GROUPS),))
    *parts, routed = pl.pallas_call(
        kernel,
        out_shape=(
            pltpu.VMEM((TOK, D), jnp.float32),
            pltpu.VMEM((LAST, D), jnp.bfloat16),
            pltpu.VMEM((TOK, LAST), jnp.bfloat16),
            pltpu.VMEM((TOK, LANES), jnp.float32),
            pltpu.SMEM((1,), jnp.int32),
        ),
        in_specs=[hbm] * 6,
        out_specs=(vmem, vmem, vmem, vmem, smem),
        scratch_shapes=[
            pltpu.VMEM((TOK, D), jnp.bfloat16),
            pltpu.VMEM((1, TOK), jnp.int32),
            pltpu.VMEM((1, TOK), jnp.float32),
            pltpu.VMEM((1, D), jnp.float32),
            pltpu.VMEM((D, FF), jnp.bfloat16),
            pltpu.VMEM((FF, D), jnp.bfloat16),
            pltpu.VMEM((TOK, D), jnp.bfloat16),
            pltpu.VMEM((TOK, LANES), jnp.int32),
            slab,
            slab,
            slab,
            slab,
            pltpu.VMEM((MOST, FF), jnp.bfloat16),
            pltpu.SemaphoreType.DMA((6,)),
            sems,
            sems,
            sems,
            sems,
        ],
        compiler_params=pltpu.CompilerParams(
            collective_id=0, has_side_effects=True, vmem_limit_bytes=VMEM_LIMIT
        ),
    )(
        *(
            pltpu.with_memory_space_constraint(a, pltpu.HBM)
            for a in (
                tokens,
                expert_ids.reshape(1, TOK),
                gate_prob.reshape(1, TOK),
                norm_gain.reshape(1, D),
                weight_in,
                weight_out,
            )
        )
    )
    return pl.pallas_call(
        finish,
        out_shape=outs,
        in_specs=[vmem, vmem, vmem, vmem, smem],
        out_specs=(hbm, hbm),
        scratch_shapes=[pltpu.VMEM((TOK, D), jnp.bfloat16), pltpu.SemaphoreType.DMA((OUT_PIECES + 1,))],
        compiler_params=pltpu.CompilerParams(vmem_limit_bytes=8 * 2**20),
    )(*parts, routed)


def solution(mesh):
    return jax.shard_map(
        on_device,
        mesh=mesh,
        in_specs=(
            P(ROW_COL, None),
            P(ROW_COL, None),
            P(ROW_COL),
            P(),
            P(ROW_COL, None, None),
            P(ROW_COL, None, None),
        ),
        out_specs=(P(ROW_COL, None), P(ROW_COL)),
        check_vma=False,
    )
```
